32 devices in a mesh: patch: 2 (over y), gz: 4 (over z), row: 4 (over x, core).
Axes of the slice: x: 2, y: 2, z: 4, core: 2. Of those that a mesh axis runs over, the one named last changes fastest.
Arguments:
- contrast: bfloat16 [32, 128, 1024], P(('patch', 'gz'), 'row'), parts along dimension 0, may hold values from -6 to 6
- lens_weight: float32 [16], P('gz'), may hold values from 0.05 to 0.5
- distances: float32 [2, 16], P(None, 'gz'), may hold values from 1.25 to 25, as said below
Outputs:
- convergence: float32 [32, 128, 1024], P(('patch', 'gz'), 'row'), parts along dimension 0
The draws below stay inside these ranges and needn't reach their ends.
There are 2 independent parts, one for each index of `patch`. The reference program is written for one: setup_inputs(seed, part) draws one part's arguments, and reference() takes and returns one part's arrays. A program takes and returns all parts, laid end to end along the dimension named above; an argument that names none is the same for every part. Nothing has to cross between parts.
Inputs may be any that keep to these rules, and one draw needn't show every extreme that they name: `distances`: both rows rise along the slices, and each slice's lens distance lies below its source distance, which lies below the next slice's lens distance.
All inputs are finite; a program needn't handle non-finite values.
Results may differ from the reference program's by a relative error of at most 0.0049.
Values may be sent and summed in bfloat16 or wider, within the bound.
A program may use at most 64 MiB of HBM per device.

```python
import math
import jax
import jax.numpy as jnp
from jax import lax

COLS = 1024
SLICES = 16
ROWS = 128


def distance_table(key):
    subkey = jax.random.fold_in(key, 11)
    increments = jax.random.uniform(subkey, (SLICES,), jnp.float32, 0.5, 1.5)
    far = 1.0 + jnp.cumsum(increments)
    near = far - 0.5 * increments
    return jnp.stack([near, far]).astype(jnp.float32)


def draw_distances(key, part):
    return distance_table(key)


def shard_levels(rng, shape, shards, low, top_value):
    loudness = 1.0
    for axis_at, shards_of in shards:
        heights = jax.random.uniform(jax.random.fold_in(jax.random.fold_in(rng, 6), axis_at), (shards_of,), jnp.float32, low / len(shards), top_value / len(shards))
        loudness = loudness * jnp.repeat(jnp.exp(heights), shape[axis_at] // shards_of).reshape((-1,) + (1,) * (len(shape) - 1 - axis_at))
    return loudness


def gaussian(stream_key, extent, spread, bound, shards=(), held_as=jnp.bfloat16):
    level = shard_levels(stream_key, extent, shards, -0.22, 0.18) if shards else 1.0
    entries = jax.random.normal(stream_key, extent, jnp.float32) * spread * level
    return jnp.minimum(jnp.maximum(entries, -bound), bound).astype(held_as)


def setup_inputs(seed: int = 0, part: int = 0) -> dict:
    arg_keys = jax.random.split(jax.random.key(seed), 4)
    part_splits = jax.random.split(jax.random.fold_in(arg_keys[3], part), 4)
    return {
        "contrast": gaussian(part_splits[0], (SLICES, ROWS, COLS), 1.0, 6.0, ((0, 4), (1, 4))),
        "lens_weight": jnp.clip(jnp.exp(math.log(0.5) - 2.3025851 * jax.random.uniform(arg_keys[1], (SLICES,), jnp.float32) ** shard_levels(arg_keys[1], (SLICES,), ((0, 4),), -0.2, 0.2)), 0.05, 0.5),
        "distances": draw_distances(jax.random.fold_in(arg_keys[3], 71), part),
    }


SMOOTH_TAPS = (0.0625, 0.1875, 0.5, 0.1875, 0.0625)

def beam_table(count):
    index = jnp.arange(count).astype(jnp.float32)
    offset = index[:, None] - index[None, :]
    return (jnp.exp(-offset * offset) / math.sqrt(math.pi)).astype(jnp.bfloat16)

def smooth_rows(padded, count):
    total = SMOOTH_TAPS[0] * padded[..., 0:count, :]
    for offset in range(1, 5):
        total = total + SMOOTH_TAPS[offset] * padded[..., offset:offset + count, :]
    return total

def reference(contrast, lens_weight, distances):
    near = distances[0]
    far = distances[1]
    beam = beam_table(contrast.shape[2])

    def advance(carry, inputs):
        sum_plain, sum_dist = carry
        slab, weight, lens_dist, source_dist = inputs
        across = jnp.dot(slab, beam, preferred_element_type=jnp.float32)
        padded = jnp.pad(across, ((2, 2), (0, 0)))
        smoothed = smooth_rows(padded, slab.shape[0])
        sum_plain = sum_plain + weight * smoothed
        sum_dist = sum_dist + weight * lens_dist * smoothed
        return ((sum_plain, sum_dist), sum_plain - sum_dist / source_dist)
    zeros = jnp.zeros(contrast.shape[1:], jnp.float32)
    ignored, maps = lax.scan(advance, (zeros, zeros), (contrast, lens_weight, near, far))
    return maps
```

```python
import functools
import math

import jax
import jax.numpy as jnp
from jax import lax
from jax.experimental import pallas as pl
from jax.experimental.pallas import tpu as pltpu
from jax.sharding import PartitionSpec as P

MESH = pl.DeviceIdType.MESH
BLOCK = 256
REACH = 128
EDGE = 8
TAPS = (0.5, 0.1875, 0.0625)


def filter_rows(x):
    count = x.shape[0]
    near = pltpu.roll(x, 1, 0) + pltpu.roll(x, count - 1, 0)
    far = pltpu.roll(x, 2, 0) + pltpu.roll(x, count - 2, 0)
    return TAPS[0] * x + TAPS[1] * near + TAPS[2] * far


def kernel(
    n_gz, n_row, c_hbm, weight_ref, dist_ref, out_ref,
    c_ref, beam_ref, acc_ref, halo_out, halo_in, dist_out, dist_in, plain_ref,
    sent, got, load_sem, halo_send, halo_recv, dist_sems, chain_send, chain_recv,
):
    slices, rows, cols = c_ref.shape
    blocks = cols // BLOCK
    chunks = 2 * blocks
    gz = lax.axis_index("gz")
    row = lax.axis_index("row")
    has_up, has_down = row > 0, row < n_row - 1
    has_prev, has_next = gz > 0, gz < n_gz - 1
    up, down = {"row": row - 1}, {"row": row + 1}
    prev, nxt = {"gz": gz - 1}, {"gz": gz + 1}

    load = pltpu.make_async_copy(c_hbm, c_ref, load_sem)
    load.start()
    barrier = pltpu.get_barrier_semaphore()
    for there, device in ((has_up, up), (has_down, down), (has_prev, prev)):
        @pl.when(there)
        def _(device=device):
            pl.semaphore_signal(barrier, inc=1, device_id=device, device_id_type=MESH)

    def halo_copy(side, device):
        return pltpu.make_async_remote_copy(
            src_ref=halo_out.at[side], dst_ref=halo_in.at[1 - side],
            send_sem=halo_send.at[side], recv_sem=halo_recv.at[1 - side],
            device_id=device, device_id_type=MESH,
        )

    def chain_copy(chunk):
        return pltpu.make_async_remote_copy(
            src_ref=sent.at[chunk], dst_ref=got.at[chunk],
            send_sem=chain_send.at[chunk], recv_sem=chain_recv.at[chunk],
            device_id=nxt, device_id_type=MESH,
        )

    dist_copy = pltpu.make_async_remote_copy(
        src_ref=dist_out, dst_ref=dist_in, send_sem=dist_sems.at[0],
        recv_sem=dist_sems.at[1], device_id=nxt, device_id_type=MESH,
    )

    dist_out[...] = jnp.full(dist_out.shape, dist_ref[1, slices - 1], jnp.float32)
    window = BLOCK + 2 * REACH
    source = lax.broadcasted_iota(jnp.int32, (window, BLOCK), 0)
    target = lax.broadcasted_iota(jnp.int32, (window, BLOCK), 1)
    offset = (source - REACH - target).astype(jnp.float32)
    beam_ref[...] = (jnp.exp(-offset * offset) / math.sqrt(math.pi)).astype(jnp.bfloat16)
    ones = jnp.ones((1, BLOCK), jnp.float32)
    weight = [ones * weight_ref[i] for i in range(slices)]
    weight_near = [weight[i] * dist_ref[0, i] for i in range(slices)]
    far = [ones * dist_ref[1, i] for i in range(slices)]
    inverse = [1.0 / far[i] for i in range(slices)]

    load.wait()
    place = lax.broadcasted_iota(jnp.int32, (2 * slices, cols), 0) // 2
    for side, start in ((0, 0), (1, rows - 2)):
        base = 0 if side == 0 else rows - 16
        packed = jnp.zeros((2 * slices, cols), jnp.float32)
        for i in range(slices):
            piece = c_ref[i, base : base + 16, :].astype(jnp.float32)
            piece = piece[0:8] if side == 0 else piece[8:16]
            piece = pltpu.roll(piece, (2 * i + (0 if side == 0 else 2)) % 8, 0)
            packed = jnp.where(place == i, piece, packed)
        halo_out[side] = packed.astype(halo_out.dtype)

    @pl.when(jnp.logical_not(has_up))
    def _():
        halo_in[0] = jnp.zeros(halo_in.shape[1:], halo_in.dtype)

    @pl.when(jnp.logical_not(has_down))
    def _():
        halo_in[1] = jnp.zeros(halo_in.shape[1:], halo_in.dtype)

    peers = sum(there.astype(jnp.int32) for there in (has_up, has_down, has_next))
    pl.semaphore_wait(barrier, peers)

    for there, side, device in ((has_up, 0, up), (has_down, 1, down)):
        @pl.when(there)
        def _(side=side, device=device):
            halo_copy(side, device).start()

    @pl.when(has_next)
    def _():
        dist_copy.start()

    def across(x, low, high, shift):
        return jnp.dot(
            x, beam_ref[low - shift : high - shift, :], preferred_element_type=jnp.float32
        )

    def span(block):
        shift = block * BLOCK - REACH
        return max(shift, 0), min(shift + window, cols), shift

    def advance(chunk, columns, parts):
        plain = jnp.zeros(parts[0].shape, jnp.float32)
        dist = jnp.zeros(parts[0].shape, jnp.float32)
        maps = []
        for i in range(slices):
            plain = plain + weight[i] * parts[i]
            dist = dist + weight_near[i] * parts[i]
            maps.append(plain - dist * inverse[i])
        put(chunk, columns, maps)
        plain_ref[chunk] = plain

        @pl.when(jnp.logical_and(has_next, jnp.logical_not(has_prev)))
        def _():
            sent[chunk, 0] = plain.astype(sent.dtype)
            sent[chunk, 1] = maps[-1].astype(sent.dtype)
            chain_copy(chunk).start()

    def put(chunk, columns, maps):
        for i in range(slices):
            if chunk < blocks:
                out_ref[i, EDGE : rows - EDGE, columns] = maps[i]
            else:
                out_ref[i, 0:EDGE, columns] = maps[i][0:EDGE]
                out_ref[i, rows - EDGE : rows, columns] = maps[i][EDGE:]

    def take(chunk, columns, i):
        if chunk < blocks:
            return out_ref[i, EDGE : rows - EDGE, columns]
        return jnp.concatenate(
            [out_ref[i, 0:EDGE, columns], out_ref[i, rows - EDGE : rows, columns]], axis=0
        )

    for block in range(blocks):
        columns = slice(block * BLOCK, (block + 1) * BLOCK)
        low, high, shift = span(block)
        flat = c_ref[:, :, low:high].reshape(slices * rows, high - low)
        acc = across(flat, low, high, shift)
        acc_ref[:, columns] = acc
        parts = [
            filter_rows(acc[i * rows : (i + 1) * rows])[EDGE : rows - EDGE]
            for i in range(slices)
        ]
        advance(block, columns, parts)

    for there, side, device in ((has_up, 0, up), (has_down, 1, down)):
        @pl.when(there)
        def _(side=side, device=device):
            halo_copy(1 - side, device).wait_recv()

    for block in range(blocks):
        columns = slice(block * BLOCK, (block + 1) * BLOCK)
        low, high, shift = span(block)
        halo = jnp.concatenate([halo_in[0, :, low:high], halo_in[1, :, low:high]], axis=0)
        halo = across(halo.astype(jnp.bfloat16), low, high, shift)
        above, below = halo[0 : 2 * slices], halo[2 * slices :]
        parts = []
        for i in range(slices):
            first, last = i * rows, (i + 1) * rows
            top = jnp.concatenate(
                [pltpu.roll(above, (6 - 2 * i) % 8, 0), acc_ref[first : first + 16, columns]],
                axis=0,
            )
            bottom = jnp.concatenate(
                [acc_ref[last - 16 : last, columns], pltpu.roll(below, (8 - 2 * i) % 8, 0)],
                axis=0,
            )
            parts.append(
                jnp.concatenate([filter_rows(top)[8:16], filter_rows(bottom)[8:16]], axis=0)
            )
        advance(blocks + block, columns, parts)

    @pl.when(has_prev)
    def _():
        dist_copy.wait_recv()
        entered = jnp.concatenate([dist_in[0:1, :]] * (BLOCK // 128), axis=1)
        ratio = [entered * inverse[i] for i in range(slices)]
        for chunk in range(chunks):
            block = chunk % blocks
            columns = slice(block * BLOCK, (block + 1) * BLOCK)
            chain_copy(chunk).wait_recv()
            before = got[chunk, 0].astype(jnp.float32)
            change = got[chunk, 1].astype(jnp.float32) - before
            maps = [
                take(chunk, columns, i) + (before + ratio[i] * change) for i in range(slices)
            ]

            @pl.when(has_next)
            def _():
                sent[chunk, 0] = (before + plain_ref[chunk]).astype(sent.dtype)
                sent[chunk, 1] = maps[-1].astype(sent.dtype)
                chain_copy(chunk).start()

            put(chunk, columns, maps)

    for there, side, device in ((has_up, 0, up), (has_down, 1, down)):
        @pl.when(there)
        def _(side=side, device=device):
            halo_copy(side, device).wait_send()

    @pl.when(has_next)
    def _():
        dist_copy.wait_send()
        for chunk in range(chunks):
            chain_copy(chunk).wait_send()


def local(n_gz, n_row, contrast, lens_weight, distances):
    slices, rows, cols = contrast.shape
    wire = jnp.bfloat16 if n_gz <= 8 else jnp.float32
    chunks = 2 * (cols // BLOCK)
    mid = rows - 2 * EDGE
    assert mid == 2 * EDGE and 2 * slices == EDGE and cols % BLOCK == 0
    return pl.pallas_call(
        functools.partial(kernel, n_gz, n_row),
        out_shape=jax.ShapeDtypeStruct((slices, rows, cols), jnp.float32),
        in_specs=[
            pl.BlockSpec(memory_space=pl.ANY),
            pl.BlockSpec(memory_space=pltpu.SMEM),
            pl.BlockSpec(memory_space=pltpu.SMEM),
        ],
        out_specs=pl.BlockSpec(memory_space=pltpu.VMEM),
        scratch_shapes=[
            pltpu.VMEM((slices, rows, cols), jnp.bfloat16),
            pltpu.VMEM((BLOCK + 2 * REACH, BLOCK), jnp.bfloat16),
            pltpu.VMEM((slices * rows, cols), jnp.float32),
            pltpu.VMEM((2, 2 * slices, cols), jnp.bfloat16),
            pltpu.VMEM((2, 2 * slices, cols), jnp.bfloat16),
            pltpu.VMEM((8, 128), jnp.float32),
            pltpu.VMEM((8, 128), jnp.float32),
            pltpu.VMEM((chunks, mid, BLOCK), jnp.float32),
            pltpu.VMEM((chunks, 2, mid, BLOCK), wire),
            pltpu.VMEM((chunks, 2, mid, BLOCK), wire),
            pltpu.SemaphoreType.DMA,
            pltpu.SemaphoreType.DMA((2,)),
            pltpu.SemaphoreType.DMA((2,)),
            pltpu.SemaphoreType.DMA((2,)),
            pltpu.SemaphoreType.DMA((chunks,)),
            pltpu.SemaphoreType.DMA((chunks,)),
        ],
        compiler_params=pltpu.CompilerParams(
            collective_id=0, has_side_effects=True, vmem_limit_bytes=8 * 1024 * 1024
        ),
    )(contrast, lens_weight, distances)


def solution(mesh):
    return jax.shard_map(
        functools.partial(local, mesh.shape["gz"], mesh.shape["row"]),
        mesh=mesh,
        in_specs=(P(("patch", "gz"), "row", None), P("gz"), P(None, "gz")),
        out_specs=P(("patch", "gz"), "row", None),
        check_vma=False,
    )
```

```python
import functools
import math

import jax
import jax.numpy as jnp
from jax import lax
from jax.experimental import pallas as pl
from jax.experimental.pallas import tpu as pltpu
from jax.sharding import PartitionSpec as P

MESH = pl.DeviceIdType.MESH
BLOCK = 256
REACH = 128
EDGE = 8
TAPS = (0.5, 0.1875, 0.0625)


def filter_rows(x):
    count = x.shape[0]
    near = pltpu.roll(x, 1, 0) + pltpu.roll(x, count - 1, 0)
    far = pltpu.roll(x, 2, 0) + pltpu.roll(x, count - 2, 0)
    return TAPS[0] * x + TAPS[1] * near + TAPS[2] * far


def kernel(
    n_gz, n_row, c_hbm, weight_hbm, dist_hbm, out_hbm,
    out_ref, weight_ref, dist_ref, c_ref, beam_ref, acc_ref, halo_out, halo_in, dist_out, dist_in, plain_ref,
    sent, got, load_sems, halo_send, halo_recv, dist_sems, chain_send, chain_recv, store_sems,
):
    slices, rows, cols = c_ref.shape
    blocks = cols // BLOCK
    chunks = 2 * blocks
    gz = lax.axis_index("gz")
    row = lax.axis_index("row")
    has_up, has_down = row > 0, row < n_row - 1
    has_prev, has_next = gz > 0, gz < n_gz - 1
    up, down = {"row": row - 1}, {"row": row + 1}
    prev, nxt = {"gz": gz - 1}, {"gz": gz + 1}

    load = pltpu.make_async_copy(c_hbm, c_ref, load_sems.at[0])
    load.start()
    small = [
        pltpu.make_async_copy(weight_hbm, weight_ref, load_sems.at[1]),
        pltpu.make_async_copy(dist_hbm, dist_ref, load_sems.at[2]),
    ]
    for copy in small:
        copy.start()
    barrier = pltpu.get_barrier_semaphore()
    for there, device in ((has_up, up), (has_down, down), (has_prev, prev)):
        @pl.when(there)
        def _(device=device):
            pl.semaphore_signal(barrier, inc=1, device_id=device, device_id_type=MESH)

    def halo_copy(side, device):
        return pltpu.make_async_remote_copy(
            src_ref=halo_out.at[side], dst_ref=halo_in.at[1 - side],
            send_sem=halo_send.at[side], recv_sem=halo_recv.at[1 - side],
            device_id=device, device_id_type=MESH,
        )

    def chain_copy(chunk):
        return pltpu.make_async_remote_copy(
            src_ref=sent.at[chunk], dst_ref=got.at[chunk],
            send_sem=chain_send.at[chunk], recv_sem=chain_recv.at[chunk],
            device_id=nxt, device_id_type=MESH,
        )

    dist_copy = pltpu.make_async_remote_copy(
        src_ref=dist_out, dst_ref=dist_in, send_sem=dist_sems.at[0],
        recv_sem=dist_sems.at[1], device_id=nxt, device_id_type=MESH,
    )

    window = BLOCK + 2 * REACH
    source = lax.broadcasted_iota(jnp.int32, (window, BLOCK), 0)
    target = lax.broadcasted_iota(jnp.int32, (window, BLOCK), 1)
    offset = (source - REACH - target).astype(jnp.float32)
    beam_ref[...] = (jnp.exp(-offset * offset) / math.sqrt(math.pi)).astype(jnp.bfloat16)
    for copy in small:
        copy.wait()
    dist_out[...] = jnp.full(dist_out.shape, dist_ref[1, slices - 1], jnp.float32)
    ones = jnp.ones((1, BLOCK), jnp.float32)
    weight = [ones * weight_ref[i] for i in range(slices)]
    weight_near = [weight[i] * dist_ref[0, i] for i in range(slices)]
    far = [ones * dist_ref[1, i] for i in range(slices)]
    inverse = [1.0 / far[i] for i in range(slices)]

    load.wait()
    place = lax.broadcasted_iota(jnp.int32, (2 * slices, cols), 0) // 2
    for side, start in ((0, 0), (1, rows - 2)):
        base = 0 if side == 0 else rows - 16
        packed = jnp.zeros((2 * slices, cols), jnp.float32)
        for i in range(slices):
            piece = c_ref[i, base : base + 16, :].astype(jnp.float32)
            piece = piece[0:8] if side == 0 else piece[8:16]
            piece = pltpu.roll(piece, (2 * i + (0 if side == 0 else 2)) % 8, 0)
            packed = jnp.where(place == i, piece, packed)
        halo_out[side] = packed.astype(halo_out.dtype)

    @pl.when(jnp.logical_not(has_up))
    def _():
        halo_in[0] = jnp.zeros(halo_in.shape[1:], halo_in.dtype)

    @pl.when(jnp.logical_not(has_down))
    def _():
        halo_in[1] = jnp.zeros(halo_in.shape[1:], halo_in.dtype)

    peers = sum(there.astype(jnp.int32) for there in (has_up, has_down, has_next))
    pl.semaphore_wait(barrier, peers)

    for there, side, device in ((has_up, 0, up), (has_down, 1, down)):
        @pl.when(there)
        def _(side=side, device=device):
            halo_copy(side, device).start()

    @pl.when(has_next)
    def _():
        dist_copy.start()

    def across(x, low, high, shift):
        return jnp.dot(
            x, beam_ref[low - shift : high - shift, :], preferred_element_type=jnp.float32
        )

    def span(block):
        shift = block * BLOCK - REACH
        return max(shift, 0), min(shift + window, cols), shift

    def advance(chunk, columns, parts):
        plain = jnp.zeros(parts[0].shape, jnp.float32)
        dist = jnp.zeros(parts[0].shape, jnp.float32)
        maps = []
        for i in range(slices):
            plain = plain + weight[i] * parts[i]
            dist = dist + weight_near[i] * parts[i]
            maps.append(plain - dist * inverse[i])

        @pl.when(jnp.logical_and(has_next, jnp.logical_not(has_prev)))
        def _():
            sent[chunk, 0] = plain.astype(sent.dtype)
            sent[chunk, 1] = maps[-1].astype(sent.dtype)
            chain_copy(chunk).start()

        put(chunk, columns, maps)
        plain_ref[chunk] = plain

        @pl.when(jnp.logical_not(has_prev))
        def _():
            for copy in stores(chunk):
                copy.start()

    def stores(chunk):
        block = chunk % blocks
        columns = slice(block * BLOCK, (block + 1) * BLOCK)
        spans = [(EDGE, rows - EDGE)] if chunk < blocks else [(0, EDGE), (rows - EDGE, rows)]
        return [
            pltpu.make_async_copy(
                out_ref.at[:, low:high, columns],
                out_hbm.at[:, low:high, columns],
                store_sems.at[chunk, side],
            )
            for side, (low, high) in enumerate(spans)
        ]

    def put(chunk, columns, maps):
        for i in range(slices):
            if chunk < blocks:
                out_ref[i, EDGE : rows - EDGE, columns] = maps[i]
            else:
                out_ref[i, 0:EDGE, columns] = maps[i][0:EDGE]
                out_ref[i, rows - EDGE : rows, columns] = maps[i][EDGE:]

    def take(chunk, columns, i):
        if chunk < blocks:
            return out_ref[i, EDGE : rows - EDGE, columns]
        return jnp.concatenate(
            [out_ref[i, 0:EDGE, columns], out_ref[i, rows - EDGE : rows, columns]], axis=0
        )

    for block in range(blocks):
        columns = slice(block * BLOCK, (block + 1) * BLOCK)
        low, high, shift = span(block)
        flat = c_ref[:, :, low:high].reshape(slices * rows, high - low)
        acc = across(flat, low, high, shift)
        acc_ref[:, columns] = acc
        parts = [
            filter_rows(acc[i * rows : (i + 1) * rows])[EDGE : rows - EDGE]
            for i in range(slices)
        ]
        advance(block, columns, parts)

    for there, side, device in ((has_up, 0, up), (has_down, 1, down)):
        @pl.when(there)
        def _(side=side, device=device):
            halo_copy(1 - side, device).wait_recv()

    for block in range(blocks):
        columns = slice(block * BLOCK, (block + 1) * BLOCK)
        low, high, shift = span(block)
        halo = jnp.concatenate([halo_in[0, :, low:high], halo_in[1, :, low:high]], axis=0)
        halo = across(halo.astype(jnp.bfloat16), low, high, shift)
        above, below = halo[0 : 2 * slices], halo[2 * slices :]
        parts = []
        for i in range(slices):
            first, last = i * rows, (i + 1) * rows
            top = jnp.concatenate(
                [pltpu.roll(above, (6 - 2 * i) % 8, 0), acc_ref[first : first + 16, columns]],
                axis=0,
            )
            bottom = jnp.concatenate(
                [acc_ref[last - 16 : last, columns], pltpu.roll(below, (8 - 2 * i) % 8, 0)],
                axis=0,
            )
            parts.append(
                jnp.concatenate([filter_rows(top)[8:16], filter_rows(bottom)[8:16]], axis=0)
            )
        advance(blocks + block, columns, parts)

    @pl.when(has_prev)
    def _():
        dist_copy.wait_recv()
        entered = jnp.concatenate([dist_in[0:1, :]] * (BLOCK // 128), axis=1)
        ratio = [entered * inverse[i] for i in range(slices)]
        for chunk in range(chunks):
            block = chunk % blocks
            columns = slice(block * BLOCK, (block + 1) * BLOCK)
            chain_copy(chunk).wait_recv()
            before = got[chunk, 0].astype(jnp.float32)
            change = got[chunk, 1].astype(jnp.float32) - before
            maps = [
                take(chunk, columns, i) + (before + ratio[i] * change) for i in range(slices)
            ]

            @pl.when(has_next)
            def _():
                sent[chunk, 0] = (before + plain_ref[chunk]).astype(sent.dtype)
                sent[chunk, 1] = maps[-1].astype(sent.dtype)
                chain_copy(chunk).start()

            put(chunk, columns, maps)
            for copy in stores(chunk):
                copy.start()

    for there, side, device in ((has_up, 0, up), (has_down, 1, down)):
        @pl.when(there)
        def _(side=side, device=device):
            halo_copy(side, device).wait_send()

    @pl.when(has_next)
    def _():
        dist_copy.wait_send()
        for chunk in range(chunks):
            chain_copy(chunk).wait_send()

    for chunk in range(chunks):
        for copy in stores(chunk):
            copy.wait()


def local(n_gz, n_row, contrast, lens_weight, distances):
    slices, rows, cols = contrast.shape
    wire = jnp.bfloat16 if n_gz <= 8 else jnp.float32
    chunks = 2 * (cols // BLOCK)
    mid = rows - 2 * EDGE
    assert mid == 2 * EDGE and 2 * slices == EDGE and cols % BLOCK == 0
    return pl.pallas_call(
        functools.partial(kernel, n_gz, n_row),
        out_shape=jax.ShapeDtypeStruct((slices, rows, cols), jnp.float32),
        in_specs=[
            pl.BlockSpec(memory_space=pl.ANY),
            pl.BlockSpec(memory_space=pl.ANY),
            pl.BlockSpec(memory_space=pl.ANY),
        ],
        out_specs=pl.BlockSpec(memory_space=pl.ANY),
        scratch_shapes=[
            pltpu.VMEM((slices, rows, cols), jnp.float32),
            pltpu.SMEM(lens_weight.shape, jnp.float32),
            pltpu.SMEM(distances.shape, jnp.float32),
            pltpu.VMEM((slices, rows, cols), jnp.bfloat16),
            pltpu.VMEM((BLOCK + 2 * REACH, BLOCK), jnp.bfloat16),
            pltpu.VMEM((slices * rows, cols), jnp.float32),
            pltpu.VMEM((2, 2 * slices, cols), jnp.bfloat16),
            pltpu.VMEM((2, 2 * slices, cols), jnp.bfloat16),
            pltpu.VMEM((8, 128), jnp.float32),
            pltpu.VMEM((8, 128), jnp.float32),
            pltpu.VMEM((chunks, mid, BLOCK), jnp.float32),
            pltpu.VMEM((chunks, 2, mid, BLOCK), wire),
            pltpu.VMEM((chunks, 2, mid, BLOCK), wire),
            pltpu.SemaphoreType.DMA((3,)),
            pltpu.SemaphoreType.DMA((2,)),
            pltpu.SemaphoreType.DMA((2,)),
            pltpu.SemaphoreType.DMA((2,)),
            pltpu.SemaphoreType.DMA((chunks,)),
            pltpu.SemaphoreType.DMA((chunks,)),
            pltpu.SemaphoreType.DMA((chunks, 2)),
        ],
        compiler_params=pltpu.CompilerParams(
            collective_id=0, has_side_effects=True, vmem_limit_bytes=59_000_000
        ),
    )(contrast, lens_weight, distances)


def solution(mesh):
    return jax.shard_map(
        functools.partial(local, mesh.shape["gz"], mesh.shape["row"]),
        mesh=mesh,
        in_specs=(P(("patch", "gz"), "row", None), P("gz"), P(None, "gz")),
        out_specs=P(("patch", "gz"), "row", None),
        check_vma=False,
    )
```
